32 devices in a mesh: ctx: 4 (over z), shard: 8 (over y, x, core).
Axes of the slice: x: 2, y: 2, z: 4, core: 2. Of those that a mesh axis runs over, the one named last changes fastest.
Arguments:
- queries: bfloat16 [4096, 3072], P('ctx', 'shard'), may hold values from -6 to 6
- keys: bfloat16 [4096, 3072], P('ctx', 'shard'), may hold values from -6 to 6
- values: bfloat16 [4096, 3072], P('ctx', 'shard'), may hold values from -6 to 6
- token_rate: float32 [4096, 8], P('ctx'), may hold values from 0.1 to 1
- gate_fast: float32 [384, 12288], P(None, 'shard'), may hold values from -0.3125 to 0.3125
- up_fast: float32 [384, 12288], P(None, 'shard'), may hold values from -0.3125 to 0.3125
- down_fast: float32 [384, 12288], P(None, 'shard'), may hold values from -0.15625 to 0.15625
Outputs:
- applied: bfloat16 [4096, 3072], P('ctx', 'shard')
- gate_new: float32 [384, 12288], P(None, 'shard')
- up_new: float32 [384, 12288], P(None, 'shard')
- down_new: float32 [384, 12288], P(None, 'shard')
The draws below stay inside these ranges and needn't reach their ends.
All inputs are finite; a program needn't handle non-finite values.
Results may differ from the reference program's by a relative error of at most 0.007.
Values may be sent and summed in bfloat16 or wider, within the bound.
No kernel may reach another device: no remote copies, remote signals or barrier semaphores. Data moves between devices by JAX's collectives and lax.ppermute only.
A program may use at most 64 MiB of HBM per device.

```python
import math
import jax
import jax.numpy as jnp
from jax import lax

HEADS = 8
DH = 384
FF = 1536
ITERS = 2
TOKENS = 4096


scale_lowest = 0.25


scale_highest = 2.4


entry_clip = 2.5


def spread_columns(key):
    scale_key, entry_key = jax.random.split(key, 2)
    column_scale = jnp.exp(jax.random.uniform(scale_key, (HEADS * DH,), jnp.float32, math.log(scale_lowest), math.log(scale_highest)))
    entries = jnp.clip(jax.random.normal(entry_key, (TOKENS, HEADS * DH), jnp.float32), -entry_clip, entry_clip)
    return (entries * column_scale[None, :]).astype(jnp.bfloat16)


def draw_keys(key, part):
    return spread_columns(jax.random.fold_in(key, 11))


def draw_values(key, part):
    return spread_columns(jax.random.fold_in(key, 23))


def block_scale(own_key, shape, pieces, least, largest):
    level, own = 1.0, jax.random.fold_in(own_key, 6)
    for dim, parts in pieces:
        draws = jnp.exp(jax.random.uniform(jax.random.fold_in(own, dim), (parts,), jnp.float32, least / len(pieces), largest / len(pieces)))
        level = level * jnp.repeat(draws, shape[dim] // parts).reshape([-1 if axis == dim else 1 for axis in range(len(shape))])
    return level


def gaussian(own_key, extent, width, bound, pieces=(), kind=jnp.bfloat16):
    values = width * jax.random.normal(own_key, extent, jnp.float32)
    if pieces:
        values = values * block_scale(own_key, extent, pieces, -0.22, 0.18)
    return jnp.clip(values, -bound, bound).astype(kind)


def setup_inputs(seed: int = 0) -> dict:
    seeds = jax.random.split(jax.random.key(seed), 8)
    queries = gaussian(seeds[0], (TOKENS, HEADS * DH), 1.0, 6.0, ((0, 4), (1, 8)))
    keys = draw_keys(jax.random.fold_in(seeds[7], 71), 0)
    values = draw_values(jax.random.fold_in(seeds[7], 71), 0)
    token_rate = jnp.clip(jnp.exp(math.log(1.0) - 2.3025851 * jax.random.uniform(seeds[3], (TOKENS, HEADS), jnp.float32) ** block_scale(seeds[3], (TOKENS, HEADS), ((0, 4),), -0.2, 0.2)), 0.1, 1.0)
    gate_fast = gaussian(seeds[4], (DH, HEADS * FF), DH ** -0.5, 0.3125, ((1, 8),), jnp.float32)
    up_fast = gaussian(seeds[5], (DH, HEADS * FF), DH ** -0.5, 0.3125, ((1, 8),), jnp.float32)
    down_fast = gaussian(seeds[6], (DH, HEADS * FF), FF ** -0.5, 0.15625, ((1, 8),), jnp.float32)
    return {"queries": queries, "keys": keys, "values": values, "token_rate": token_rate, "gate_fast": gate_fast, "up_fast": up_fast, "down_fast": down_fast}


linear_coefficient = 3.4445
square_coefficient = -4.775
cubic_coefficient = 2.0315
epsilon = 1e-06
update_factor = 0.5

def orthogonalize(gradient):
    highest = lax.Precision.HIGHEST
    squares = jnp.sum(gradient * gradient)
    current = gradient / jnp.sqrt(squares + epsilon)
    for iteration in range(ITERS):
        gram = jnp.dot(current, current.T, precision=highest)
        mixed = square_coefficient * gram + cubic_coefficient * jnp.dot(gram, gram, precision=highest)
        current = linear_coefficient * current + jnp.dot(mixed, current, precision=highest)
    return current

def contract_rows(left, right):
    return lax.dot_general(left, right, (((0,), (0,)), ((), ())), preferred_element_type=jnp.float32)

def reference(queries, keys, values, token_rate, gate_fast, up_fast, down_fast):
    outputs = []
    gate_list = []
    up_list = []
    down_list = []
    for head_index in range(HEADS):
        columns = slice(head_index * DH, (head_index + 1) * DH)
        hidden_cols = slice(head_index * FF, (head_index + 1) * FF)
        gate_w = gate_fast[:, hidden_cols]
        up_w = up_fast[:, hidden_cols]
        down_w = down_fast[:, hidden_cols]
        gate_bf = gate_w.astype(jnp.bfloat16)
        up_bf = up_w.astype(jnp.bfloat16)
        down_bf = down_w.astype(jnp.bfloat16)
        query_rows = queries[:, columns]
        key_rows = keys[:, columns]
        value_rows = values[:, columns]
        qgate = jnp.dot(query_rows, gate_bf, preferred_element_type=jnp.float32)
        qup = jnp.dot(query_rows, up_bf, preferred_element_type=jnp.float32)
        qhidden = (jax.nn.silu(qgate) * qup).astype(jnp.bfloat16)
        result = lax.dot_general(qhidden, down_bf, (((1,), (1,)), ((), ())), preferred_element_type=jnp.float32)
        outputs.append(result.astype(jnp.bfloat16))
        kgate = jnp.dot(key_rows, gate_bf, preferred_element_type=jnp.float32)
        kup = jnp.dot(key_rows, up_bf, preferred_element_type=jnp.float32)
        sigma = jax.nn.sigmoid(kgate)
        active = kgate * sigma
        khidden = (active * kup).astype(jnp.bfloat16)
        weighted = (value_rows.astype(jnp.float32) * token_rate[:, head_index:head_index + 1]).astype(jnp.bfloat16)
        backward = jnp.dot(weighted, down_bf, preferred_element_type=jnp.float32)
        dgate = (backward * kup * sigma * (1.0 + kgate * (1.0 - sigma))).astype(jnp.bfloat16)
        dup = (backward * active).astype(jnp.bfloat16)
        grad_gate = contract_rows(key_rows, dgate)
        grad_up = contract_rows(key_rows, dup)
        grad_down = contract_rows(weighted, khidden)
        gate_list.append(gate_w + update_factor * orthogonalize(grad_gate))
        up_list.append(up_w + update_factor * orthogonalize(grad_up))
        down_list.append(down_w + update_factor * orthogonalize(grad_down))
    applied = jnp.concatenate(outputs, axis=1)
    return (applied, jnp.concatenate(gate_list, axis=1), jnp.concatenate(up_list, axis=1), jnp.concatenate(down_list, axis=1))
```

```python
import functools

import jax
import jax.numpy as jnp
from jax import lax
from jax.experimental import pallas as pl
from jax.experimental.pallas import tpu as pltpu
from jax.sharding import PartitionSpec as P


HEADS = 8
ITERS = 2


linear_coefficient = 3.4445
square_coefficient = -4.775
cubic_coefficient = 2.0315
epsilon = 1e-06
update_factor = 0.5

MIB = 1 << 20
F32 = jnp.float32
BF16 = jnp.bfloat16
VMEM = pltpu.VMEM
LAG = 3


def dot(a, b, dims=((1,), (0,))):
    return lax.dot_general(a, b, (dims, ((), ())), preferred_element_type=F32)


def sigmoid(x):
    return 0.5 * (1.0 + jnp.tanh(0.5 * x))


def token_block(tokens):
    return 256 if tokens % 256 == 0 else tokens


def fetch(copies, sems):
    started = [pltpu.make_async_copy(src, dst, sems.at[n]) for n, (src, dst) in enumerate(copies)]
    for copy in started:
        copy.start()
    return started


def first_kernel(head_ref, z_ref, rate_hbm, k_hbm, v_hbm, w1_hbm, w3_hbm, end_ref, g2_ref, k_ref, pv_ref, pvt_ref, kt_ref, kh, rate, v, w1f, w3f, w1, w3, sems):
    tokens = k_ref.shape[0]
    width = g2_ref.shape[1]
    end_ref[0] = jnp.where((z_ref[0] == 0) | (z_ref[0] == 3), 1, 0)
    block = token_block(tokens)
    columns = pl.ds(0, width)
    got_k, got_w1, got_w3, got_v, got_rate = fetch(
        (
            (k_hbm, k_ref),
            (w1_hbm.at[:, columns], w1f),
            (w3_hbm.at[:, columns], w3f),
            (v_hbm, v),
            (rate_hbm, rate),
        ),
        sems,
    )
    got_w1.wait()
    w1[...] = w1f[...].astype(BF16)
    got_w3.wait()
    w3[...] = w3f[...].astype(BF16)
    got_k.wait()
    got_v.wait()
    got_rate.wait()
    row = rate[pl.ds(head_ref[0], 1), :]
    eta = jnp.broadcast_to(row, (8, tokens))
    rate[...] = eta

    @pl.loop(0, tokens // block)
    def _(t):
        rows = pl.ds(pl.multiple_of(t * block, block), block)
        k = k_ref[rows, :]
        gate = dot(k, w1[...])
        up = dot(k, w3[...])
        kt_ref[:, rows] = k.T
        column = rate[:, rows].T[:, :1]
        pv = (v[rows, :].astype(F32) * column).astype(BF16)
        pv_ref[rows, :] = pv
        pvt_ref[:, rows] = pv.T
        kh[rows, :] = (gate * sigmoid(gate) * up).astype(BF16)

    g2_ref[...] = dot(pvt_ref[...], kh[...]).astype(BF16)


def keys_kernel(want, column, k_ref, pv_ref, pvt_ref, kt_ref, w1_hbm, w3_hbm, w2_hbm, *rest):
    outs, (kh, dg, du, w1f, w3f, w2f, sems) = rest[:-7], rest[-7:]
    w1_out, w3_out, w2_out = outs[:3]
    tokens = k_ref.shape[0]
    block = token_block(tokens)
    width = w1_out.shape[1]
    columns = pl.ds(column * width, width)
    copies = fetch(
        [(w.at[:, columns], f) for w, f in ((w1_hbm, w1f), (w3_hbm, w3f), (w2_hbm, w2f))], sems
    )
    for copy, out, f in zip(copies, (w1_out, w3_out, w2_out), (w1f, w3f, w2f)):
        copy.wait()
        out[...] = f[...].astype(BF16)

    @pl.loop(0, tokens // block)
    def _(t):
        rows = pl.ds(pl.multiple_of(t * block, block), block)
        k = k_ref[rows, :]
        gate = dot(k, w1_out[...])
        up = dot(k, w3_out[...])
        back = dot(pv_ref[rows, :], w2_out[...])
        s = sigmoid(gate)
        act = gate * s
        if "g2" in want:
            kh[rows, :] = (act * up).astype(BF16)
        dg[rows, :] = (back * up * s * (1.0 + gate * (1.0 - s))).astype(BF16)
        du[rows, :] = (back * act).astype(BF16)

    for name, out in zip(want, outs[3:]):
        left, right = {"g2": (pvt_ref, kh), "g1": (kt_ref, dg), "g3": (kt_ref, du)}[name]
        out[...] = dot(left[...], right[...]).astype(BF16)


def queries_kernel(blocks, part, q_hbm, *rest):
    w1, w3, w2 = rest[:blocks], rest[blocks : 2 * blocks], rest[2 * blocks : 3 * blocks]
    out_hbm, q, out, sems = rest[-4:]
    count = q.shape[0]
    rows = pl.ds(part * count, count)
    fetch([(q_hbm.at[rows, :], q)], sems)[0].wait()
    total = None
    for i in range(blocks):
        gate = dot(q[...], w1[i][...])
        up = dot(q[...], w3[i][...])
        hidden = (gate * sigmoid(gate) * up).astype(BF16)
        part = dot(hidden, w2[i][...], ((1,), (1,)))
        total = part if total is None else total + part
    out[...] = total.astype(BF16)
    copy = pltpu.make_async_copy(out, out_hbm.at[rows, :], sems.at[1])
    copy.start()
    copy.wait()


def add_kernel(own_ref, got_ref, out_ref):
    out_ref[...] = (own_ref[...].astype(F32) + got_ref[...].astype(F32)).astype(BF16)


def forward_kernel(end_ref, own_ref, got_ref, next_ref, total_ref, send_ref):
    total = (own_ref[...].astype(F32) + got_ref[...].astype(F32)).astype(BF16)
    total_ref[...] = total

    @pl.when(end_ref[0] == 1)
    def _():
        send_ref[...] = next_ref[...]

    @pl.when(end_ref[0] == 0)
    def _():
        send_ref[...] = total


def coarse(a, b):
    return dot(a.astype(BF16), b.astype(BF16))


def polynomial(first):
    row = lax.broadcasted_iota(jnp.int32, first.shape, 0)
    col = lax.broadcasted_iota(jnp.int32, first.shape, 1)
    diagonal = row == col
    squares = jnp.sum(jnp.where(diagonal, first, 0.0))
    scale = lax.rsqrt(jnp.full((1, 1), squares + epsilon, F32))
    first = first * (scale * scale)
    poly = None
    for _ in range(ITERS):
        gram = first if poly is None else coarse(coarse(poly, first), poly)
        mixed = square_coefficient * gram + cubic_coefficient * coarse(gram, gram)
        mixed = mixed + jnp.where(diagonal, linear_coefficient, 0.0)
        poly = mixed if poly is None else coarse(mixed, poly)
    return poly * (scale * update_factor)


def newton_kernel(blocks, end_ref, *rest):
    ours, theirs = rest[:blocks], rest[blocks : 2 * blocks]
    w_hbm, out_hbm, w, out, sems_in, sems_out = rest[2 * blocks :]
    width = ours[0].shape[1]
    places = [(slice(None), pl.ds(i * width, width)) for i in range(blocks)]
    arriving = fetch([(w_hbm.at[place], w.at[i]) for i, place in enumerate(places)], sems_in)

    def run(g):
        first = None
        for i in range(blocks):
            part = dot(g[i][...], g[i][...], ((1,), (1,)))
            first = part if first is None else first + part
        factor = polynomial(first).astype(BF16)
        for i in range(blocks):
            arriving[i].wait()
            out[i] = w[i] + dot(factor, g[i][...])
            pltpu.make_async_copy(out.at[i], out_hbm.at[places[i]], sems_out.at[i]).start()

    @pl.when(end_ref[0] == 1)
    def _():
        run(theirs)

    @pl.when(end_ref[0] == 0)
    def _():
        run(ours)

    for i in range(blocks):
        pltpu.make_async_copy(out.at[i], out_hbm.at[places[i]], sems_out.at[i]).wait()


SMEM_SPEC = pl.BlockSpec(memory_space=pltpu.SMEM)
WHOLE = pl.BlockSpec(memory_space=VMEM)
HBM_SPEC = pl.BlockSpec(memory_space=pltpu.HBM)


def in_hbm(arrays):
    return jax.tree.map(lambda x: pltpu.with_memory_space_constraint(x, pltpu.HBM), arrays)


def cost(flops, nbytes=0):
    return pl.CostEstimate(flops=int(flops), bytes_accessed=int(nbytes), transcendentals=0)


def width_of(hidden):
    return next(w for w in (512, 384, 256, 128, hidden) if hidden % w == 0)


def plan(hidden):
    blocks = hidden // width_of(hidden)
    first = [("g2", c) for c in range(blocks)]
    order = list(range(1, blocks)) + [0]
    chunks = first + [(m, c) for m in ("g1", "g3") for c in order]
    return blocks, chunks


def schedule(blocks, chunks):
    count = len(chunks)
    fill = {}
    fill[0] = ["kb1"] if blocks > 1 else ["kb0"]
    work = [f"kb{c}" for c in range(2, blocks)] + (["kb0"] if blocks > 1 else [])
    work += [("q0", "q1"), ("q2", "q3")]
    for r in range(1, count + LAG + 1):
        step = work.pop(0) if work else ()
        fill[r] = [step] if isinstance(step, str) else list(step)
    for n, m in enumerate(("g2", "g1")):
        fill[(n + 1) * blocks - 1 + LAG + 1].append("ns_" + m)
    steps = ["first"]
    for r in range(count + LAG + 1):
        if r < count + LAG:
            steps.append(f"e{r}")
        if 1 <= r <= count:
            steps += [f"a{r - 1}", f"i{r - 1}"]
        steps += fill[r]
        if 2 <= r <= count + 1:
            steps.append(f"b{r - 2}")
    steps.append("ns_g3")
    return steps


UP = [(0, 1), (3, 2)]
DOWN = [(1, 0), (2, 3)]
BOTH = UP + DOWN
INNER = [(1, 2), (2, 1)]


def line_of_four(queries, keys, values, token_rate, gate_fast, up_fast, down_fast):
    tokens, dim = keys.shape
    hidden = gate_fast.shape[1]
    width = width_of(hidden)
    blocks, chunks = plan(hidden)
    count = len(chunks)
    steps = schedule(blocks, chunks)
    z = lax.axis_index("ctx").astype(jnp.int32).reshape(1)
    head = lax.axis_index("shard").astype(jnp.int32).reshape(1)
    chunk_shape = jax.ShapeDtypeStruct((dim, width), BF16)
    unit = 2 * tokens * dim * width
    made = {}
    grad = {}
    got, pair_sum, inner, total, send = {}, {}, {}, {}, {}
    done = {}

    def params(mib):
        return pltpu.CompilerParams(vmem_limit_bytes=int(mib * MIB))

    def run_first():
        return pl.pallas_call(
            first_kernel,
            in_specs=[SMEM_SPEC] * 2 + [HBM_SPEC] * 5,
            out_specs=[SMEM_SPEC] + [WHOLE] * 5,
            out_shape=[jax.ShapeDtypeStruct((1,), jnp.int32), chunk_shape] + [jax.ShapeDtypeStruct(x, BF16) for x in (keys.shape, keys.shape, keys.shape[::-1], keys.shape[::-1])],
            scratch_shapes=[
                VMEM((tokens, width), BF16),
                VMEM(token_rate.shape[::-1], F32),
                VMEM((tokens, dim), BF16),
                VMEM((dim, width), F32),
                VMEM((dim, width), F32),
                VMEM((dim, width), BF16),
                VMEM((dim, width), BF16),
                pltpu.SemaphoreType.DMA((5,)),
            ],
            compiler_params=params(16),
            cost_estimate=cost(3 * unit),
            name="first",
        )(head, z, in_hbm(token_rate.T), in_hbm(keys), in_hbm(values), *in_hbm((gate_fast, up_fast)))

    def run_keys(c):
        want = ("g1", "g3") if c == 0 else ("g2", "g1", "g3")
        outs = pl.pallas_call(
            functools.partial(keys_kernel, want, c),
            in_specs=[WHOLE] * 4 + [HBM_SPEC] * 3,
            out_specs=[WHOLE] * (3 + len(want)),
            out_shape=[chunk_shape] * (3 + len(want)),
            scratch_shapes=[VMEM((tokens, width), BF16)] * 3 + [VMEM((dim, width), F32)] * 3 + [pltpu.SemaphoreType.DMA((3,))],
            compiler_params=params(16),
            cost_estimate=cost((3 + len(want)) * unit),
            name="keys",
        )(made["k"], made["pv"], made["pvt"], made["kt"], *in_hbm((gate_fast, up_fast, down_fast)))
        made["w", c] = outs[:3]
        for name, value in zip(want, outs[3:]):
            grad[name, c] = value

    def run_queries(j):
        rows = tokens // 4
        weights = [made["w", c][n] for n in range(3) for c in range(blocks)]
        before = [made[f"q{j - 1}"]] if j else []
        return pl.pallas_call(
            functools.partial(queries_kernel, blocks, j),
            in_specs=[HBM_SPEC] + [WHOLE] * (3 * blocks) + [HBM_SPEC] * len(before),
            out_specs=HBM_SPEC,
            out_shape=jax.ShapeDtypeStruct((tokens, dim), BF16),
            scratch_shapes=[VMEM((rows, dim), BF16), VMEM((rows, dim), BF16), pltpu.SemaphoreType.DMA((2,))],
            input_output_aliases={1 + 3 * blocks: 0} if before else {},
            compiler_params=params(8),
            cost_estimate=cost(3 * unit * blocks // 4),
            name="queries",
        )(in_hbm(queries), *weights, *before)

    def run_newton(m, weight):
        places = [chunks.index((m, c)) for c in range(blocks)]
        return pl.pallas_call(
            functools.partial(newton_kernel, blocks),
            in_specs=[SMEM_SPEC] + [WHOLE] * (2 * blocks) + [HBM_SPEC],
            out_specs=HBM_SPEC,
            out_shape=jax.ShapeDtypeStruct(weight.shape, weight.dtype),
            scratch_shapes=[VMEM((blocks, dim, width), F32)] * 2 + [pltpu.SemaphoreType.DMA((blocks,))] * 2,
            compiler_params=params(12),
            cost_estimate=cost(4 * unit),
            name="newton",
        )(made["end"], *[total[p] for p in places], *[got[p + LAG] for p in places], in_hbm(weight))

    def run_add(p):
        return pl.pallas_call(
            add_kernel,
            in_specs=[WHOLE] * 2,
            out_specs=WHOLE,
            out_shape=chunk_shape,
            compiler_params=params(2),
            cost_estimate=cost(dim * width),
            name="add",
        )(grad[chunks[p]], got[p])

    def run_forward(p):
        after = p + LAG
        following = grad[chunks[after]] if after < count else pair_sum[p]
        return pl.pallas_call(
            forward_kernel,
            in_specs=[SMEM_SPEC] + [WHOLE] * 3,
            out_specs=[WHOLE] * 2,
            out_shape=[chunk_shape] * 2,
            compiler_params=params(2),
            cost_estimate=cost(dim * width),
            name="forward",
        )(made["end"], pair_sum[p], inner[p], following)

    for step in steps:
        if step == "first":
            made["end"], grad["g2", 0], made["k"], made["pv"], made["pvt"], made["kt"] = run_first()
        elif step.startswith("kb"):
            run_keys(int(step[2:]))
        elif step.startswith("q"):
            made[step] = run_queries(int(step[1:]))
        elif step.startswith("ns_"):
            m = step[3:]
            done[m] = run_newton(m, {"g1": gate_fast, "g3": up_fast, "g2": down_fast}[m])
        else:
            p = int(step[1:])
            if step[0] == "e":
                if p < LAG:
                    got[p] = lax.ppermute(grad[chunks[p]], "ctx", UP)
                else:
                    got[p] = lax.ppermute(send[p], "ctx", BOTH if p < count else DOWN)
            elif step[0] == "a":
                pair_sum[p] = run_add(p)
            elif step[0] == "i":
                inner[p] = lax.ppermute(pair_sum[p], "ctx", INNER)
            else:
                total[p], send[p + LAG] = run_forward(p)
    return made["q3"], done["g1"], done["g3"], done["g2"]


def from_partner(block, axis, distance):
    count = lax.axis_size(axis)
    route = []
    for low in range(count):
        high = low | 1 << distance
        if high != low and high < count:
            route += [(low, high), (high, low)]
    return lax.ppermute(block, axis, route)


def shortened(x):
    return jax.tree.map(lambda a: a.astype(jnp.bfloat16) if a.dtype == jnp.float32 else a, x)


def contract_rows(left, right):
    return lax.dot_general(left, right, (((0,), (0,)), ((), ())), preferred_element_type=jnp.float32)


def batched(form, left, right):
    return jnp.einsum(form, left, right, precision=lax.Precision.HIGHEST)


def per_device(queries, keys, values, token_rate, gate_fast, up_fast, down_fast):
    group_size = lax.axis_size("shard") // HEADS
    level_count = group_size.bit_length() - 1
    position = lax.axis_index("shard")
    head_index = position // group_size
    member = position % group_size
    stacked = jnp.stack((queries, keys, values))
    for level in range(level_count):
        partner = from_partner(stacked, "shard", level)
        upper_side = member // 2**level % 2 == 1
        stacked = jnp.where(
            upper_side,
            jnp.concatenate((partner, stacked), 2),
            jnp.concatenate((stacked, partner), 2),
        )
    query_rows = stacked[0]
    key_rows = stacked[1]
    value_rows = stacked[2]
    gate_bf = gate_fast.astype(jnp.bfloat16)
    up_bf = up_fast.astype(jnp.bfloat16)
    down_bf = down_fast.astype(jnp.bfloat16)
    qgate = jnp.dot(query_rows, gate_bf, preferred_element_type=jnp.float32)
    qup = jnp.dot(query_rows, up_bf, preferred_element_type=jnp.float32)
    qhidden = (jax.nn.silu(qgate) * qup).astype(jnp.bfloat16)
    partial_value = lax.dot_general(
        qhidden, down_bf, (((1,), (1,)), ((), ())), preferred_element_type=jnp.float32
    )
    for level in reversed(range(level_count)):
        half_width = partial_value.shape[1] // 2
        upper_side = member // 2**level % 2 == 1
        kept = jnp.where(upper_side, partial_value[:, half_width:], partial_value[:, :half_width])
        outgoing = jnp.where(
            upper_side, partial_value[:, :half_width], partial_value[:, half_width:]
        )
        partial_value = kept + from_partner(outgoing, "shard", level)
    applied = partial_value.astype(jnp.bfloat16)
    kgate = jnp.dot(key_rows, gate_bf, preferred_element_type=jnp.float32)
    kup = jnp.dot(key_rows, up_bf, preferred_element_type=jnp.float32)
    sigma = jax.nn.sigmoid(kgate)
    active = kgate * sigma
    khidden = (active * kup).astype(jnp.bfloat16)
    rate_column = lax.dynamic_slice_in_dim(token_rate, head_index, 1, 1)
    weighted = (value_rows.astype(jnp.float32) * rate_column).astype(jnp.bfloat16)
    backward = jnp.dot(weighted, down_bf, preferred_element_type=jnp.float32)
    dgate = (backward * kup * sigma * (1.0 + kgate * (1.0 - sigma))).astype(jnp.bfloat16)
    dup = (backward * active).astype(jnp.bfloat16)
    gradients = jnp.stack(
        (
            contract_rows(key_rows, dgate),
            contract_rows(key_rows, dup),
            contract_rows(weighted, khidden),
        )
    )
    gradients = lax.psum(gradients.astype(jnp.bfloat16), "ctx").astype(jnp.float32)
    first = batched("mik,mjk->mij", gradients, gradients)
    for level in range(level_count):
        first = first + from_partner(shortened(first), "shard", level).astype(first.dtype)
    squares = jnp.trace(first, axis1=1, axis2=2)
    scaling = 1.0 / jnp.sqrt(squares + epsilon)
    first = first * (scaling * scaling)[:, None, None]
    identity = jnp.eye(first.shape[1], dtype=jnp.float32)
    poly = jnp.broadcast_to(identity, first.shape)
    for _ in range(ITERS):
        gram = batched("mij,mjk->mik", batched("mij,mjk->mik", poly, first), poly)
        mixed = square_coefficient * gram + cubic_coefficient * batched("mij,mjk->mik", gram, gram)
        poly = linear_coefficient * poly + batched("mij,mjk->mik", mixed, poly)
    current = batched("mij,mjk->mik", poly, gradients) * scaling[:, None, None]
    gate_new = gate_fast + update_factor * current[0]
    up_new = up_fast + update_factor * current[1]
    down_new = down_fast + update_factor * current[2]
    return (applied, gate_new, up_new, down_new)


def solution(mesh):
    line = mesh.shape["ctx"] == 4 and mesh.shape["shard"] == HEADS

    def body(*args):
        if not line:
            return per_device(*args)
        return line_of_four(*args)

    def mapped(*args):
        return jax.shard_map(
            body,
            mesh=mesh,
            in_specs=(
                P("ctx", "shard"),
                P("ctx", "shard"),
                P("ctx", "shard"),
                P("ctx", None),
                P(None, "shard"),
                P(None, "shard"),
                P(None, "shard"),
            ),
            out_specs=(P("ctx", "shard"), P(None, "shard"), P(None, "shard"), P(None, "shard")),
            check_vma=False,
        )(*args)

    return mapped
```
